256 devices in a mesh: grating: 2 (over z), layer: 8 (over x), harm: 16 (over y, core).
Axes of the slice: x: 8, y: 8, z: 2, core: 2. Of those that a mesh axis runs over, the one named last changes fastest.
The devices are a block of a 8x8x16 slice.
Arguments:
- panels: float32 [16, 1280, 2, 640], P(('grating', 'layer'), 'harm'), parts along dimension 0, may hold values from -6 to 6
- factors: float32 [32, 1280, 2, 1280], P(('grating', 'layer'), 'harm'), parts along dimension 0, may hold values from -0.25 to 0.25
- decay: float32 [32, 1280], P(('grating', 'layer'), 'harm'), parts along dimension 0, may hold values from 0.25 to 1
- phase: float32 [32, 1280], P(('grating', 'layer'), 'harm'), parts along dimension 0, may hold values from -3.140625 to 3.140625
- kept: int32 [32], P(('grating', 'layer')), parts along dimension 0, may hold values from 640 to 1280
- start: int32 [16], P(('grating', 'layer')), parts along dimension 0, may hold values from 0 to 1
Outputs:
- advanced: float32 [16, 1280, 2, 640], P(('grating', 'layer'), 'harm'), parts along dimension 0
The draws below stay inside these ranges and needn't reach their ends.
There are 2 independent parts, one for each index of `grating`. The reference program is written for one: setup_inputs(seed, part) draws one part's arguments, and reference() takes and returns one part's arrays. A program takes and returns all parts, laid end to end along the dimension named above; each array names one. Nothing has to cross between parts.
All inputs are finite; a program needn't handle non-finite values.
Results may differ from the reference program's by a relative error of at most 0.00024.
Values sent between devices are 32-bit elements; how exact they have to be, the bound alone decides.
No kernel may reach another device: no remote copies, remote signals or barrier semaphores. Data moves between devices by JAX's collectives and lax.ppermute only.
A program may use at most 128 MiB of HBM per device.

```python
import math
import jax
import jax.numpy as jnp
from jax import lax

HARM = 1280
COLS = 640
LAYER_DEV = 2
LAYERS = 16
PANELS = 8


def with_ends(array, key, smallest, largest):
    shape = array.shape
    place = [jax.random.randint(jax.random.fold_in(key, axis), (), 0, shape[axis]) for axis in range(len(shape))]
    array = array.at[tuple(place)].set(smallest)
    longest = shape.index(max(shape))
    place[longest] = (place[longest] + 1) % shape[longest]
    return array.at[tuple(place)].set(largest)


def shard_levels(own_key, shape, shards, low, high):
    def one(dim, parts):
        heights = jax.random.uniform(jax.random.fold_in(jax.random.fold_in(own_key, 6), dim), (parts,), jnp.float32, low / len(shards), high / len(shards))
        return jnp.repeat(jnp.exp(heights), shape[dim] // parts).reshape((-1,) + (1,) * (len(shape) - dim - 1))

    level = one(*shards[0])
    for cut in shards[1:]:
        level = level * one(*cut)
    return level


def gaussian(rng, extent, scale, bound, split=(), dtype=jnp.bfloat16):
    array = scale * jax.random.normal(rng, extent, jnp.float32)
    if split:
        array = array * shard_levels(rng, extent, split, -0.22, 0.18)
    return jnp.clip(array, -bound, bound).astype(dtype)


def setup_inputs(seed: int = 0, part: int = 0) -> dict:
    arg_keys = jax.random.split(jax.random.key(seed), 7)
    part_keys = jax.random.split(jax.random.fold_in(arg_keys[6], part), 7)
    return {
        "panels": gaussian(part_keys[0], (PANELS, HARM, 2, COLS), 1.0, 6.0, ((0, 8), (1, 16)), jnp.float32),
        "factors": gaussian(part_keys[1], (LAYERS, HARM, 2, HARM), (HARM // 2) ** -0.5, 0.25, ((0, 8), (1, 16)), jnp.float32),
        "decay": jnp.clip(jnp.exp(math.log(1.0) - 1.3862944 * jax.random.uniform(part_keys[2], (LAYERS, HARM), jnp.float32) ** shard_levels(part_keys[2], (LAYERS, HARM), ((0, 8), (1, 16)), -0.2, 0.2)), 0.25, 1.0),
        "phase": jnp.clip(jax.random.uniform(part_keys[3], (LAYERS, HARM), jnp.float32, -3.140625, 3.140625), -3.140625, 3.140625),
        "kept": with_ends(jax.random.randint(part_keys[4], (LAYERS,), HARM // 2, HARM + 1), jax.random.fold_in(part_keys[4], 1), HARM // 2, HARM).astype(jnp.int32),
        "start": with_ends(jax.random.randint(part_keys[5], (PANELS,), 0, LAYER_DEV), jax.random.fold_in(part_keys[5], 1), 0, LAYER_DEV - 1).astype(jnp.int32),
    }


def contract(left_matrix, right_matrix):
    return jnp.dot(left_matrix.T, right_matrix, precision=lax.Precision.HIGHEST, preferred_element_type=jnp.float32)


def reference(panels, factors, decay, phase, kept, start):
    harmonic_index = lax.iota(jnp.int32, HARM)
    finished = []
    for group_id in range(PANELS):
        current = panels[group_id]
        for section_step in range(LAYER_DEV):
            layer_id = (group_id * LAYER_DEV + (start[group_id] + section_step) % LAYER_DEV).astype(jnp.int32)
            factor_block = factors[layer_id]
            live_rows = (harmonic_index < kept[layer_id]).astype(jnp.float32)
            magnitude = decay[layer_id] * live_rows
            prop_real = (magnitude * jnp.cos(phase[layer_id]))[:, None]
            prop_imag = (magnitude * jnp.sin(phase[layer_id]))[:, None]
            real_in = prop_real * current[:, 0] - prop_imag * current[:, 1]
            imag_in = prop_real * current[:, 1] + prop_imag * current[:, 0]
            real_out = contract(factor_block[:, 0], real_in) - contract(factor_block[:, 1], imag_in)
            imag_out = contract(factor_block[:, 0], imag_in) + contract(factor_block[:, 1], real_in)
            current = jnp.stack([real_out, imag_out], 1)
        finished.append(current)
    return jnp.roll(jnp.stack(finished), 1, axis=0)
```

```python
import jax
import jax.numpy as jnp
from jax import lax
from jax.sharding import PartitionSpec as P

PAIR = 2
CHUNKS = (128, 192)


def split(x):
    high = lax.reduce_precision(x, 8, 7)
    return high.astype(jnp.bfloat16), (x - high).astype(jnp.bfloat16)


def product(left, right):
    left_high, left_low = left
    right_high, right_low = split(right)
    return lax.dot_general(
        jnp.concatenate([left_high, left_high, left_low], 0),
        jnp.concatenate([right_high, right_low, right_high], 0),
        (((0,), (0,)), ((), ())),
        preferred_element_type=jnp.float32,
    )


def on_device(panels, factors, decay, phase, kept, start):
    depth, rows, _, outs = factors.shape
    cols = panels.shape[3]
    size = lax.axis_size("harm")
    layers = lax.axis_size("layer")
    chips = size // PAIR
    block = rows * PAIR
    half = cols // PAIR
    me = lax.axis_index("harm")
    chip = me // PAIR
    core = me % PAIR
    sign = 1 - 2 * core
    far = chips // 2
    near = chips - 1 - far

    partner = [(h, h ^ 1) for h in range(size)]

    def place(y, c):
        return (y % chips) * PAIR + c

    ahead = [(place(y, c), place(y + 1 - 2 * c, c)) for y in range(chips) for c in range(PAIR)]
    behind = [(b, a) for a, b in ahead]

    def handed(own):
        return [
            (x * size + place(y, c), (x + 1) % layers * size + place(y, c if own else 1 - c))
            for x in range(layers)
            for y in range(chips)
            for c in range(PAIR)
        ]

    swap = lambda a: lax.ppermute(a, "harm", partner)
    other_panels = swap(panels[0])
    other_factors = swap(factors)
    other_decay = swap(decay)
    other_phase = swap(phase)

    pieces = []
    offset = 0
    for width in CHUNKS:
        pieces.append((offset, width))
        offset += width
    assert offset == half

    first = core == 0
    both = jnp.concatenate([panels[0], other_panels], 0)
    mine = jnp.where(first, both[:, :, :half], both[:, :, half:])
    current = [(mine[:, 0, o : o + w], mine[:, 1, o : o + w]) for o, w in pieces]

    row = lax.iota(jnp.int32, rows)
    for step in range(depth):
        layer = (start[0] + step) % depth
        pick = lambda a: lax.dynamic_index_in_dim(a, layer, 0, keepdims=False)
        live = lambda h: (h * rows + row < kept[layer]).astype(jnp.float32)
        mag = jnp.concatenate([pick(decay) * live(me), pick(other_decay) * live(me ^ 1)])
        ang = jnp.concatenate([pick(phase), pick(other_phase)])
        pr = (mag * jnp.cos(ang))[:, None]
        pi = (mag * jnp.sin(ang))[:, None]
        own, oth = pick(factors), pick(other_factors)
        stored = jnp.concatenate([own[:, 0], oth[:, 0], own[:, 1], oth[:, 1]], 0)
        stored = split(stored)
        partial = []
        for re, im in current:
            vr = pr * re - pi * im
            vi = pr * im + pi * re
            panel = jnp.concatenate(
                [jnp.concatenate([vr, vi], 1), jnp.concatenate([-vi, vr], 1)], 0
            )
            partial.append(product(stored, panel))
        at = lambda p, d: lax.dynamic_slice_in_dim(p, (chip + d) % chips * block, block, 0)
        done = [None] * len(pieces)
        longs = [None] * len(pieces)
        shorts = [None] * len(pieces)
        for hop in range(far):
            for i, p in enumerate(partial):
                send = at(p, sign * (far - hop))
                if hop:
                    send = send + longs[i]
                longs[i] = lax.ppermute(send, "harm", ahead)
                if hop < near:
                    send = at(p, -sign * (near - hop))
                    if hop:
                        send = send + shorts[i]
                    shorts[i] = lax.ppermute(send, "harm", behind)
        done = [at(p, 0) + longs[i] + shorts[i] for i, p in enumerate(partial)]
        if step < depth - 1:
            turned = [jnp.where(first, d, jnp.concatenate([d[rows:], d[:rows]], 0)) for d in done]
            current = [(d[:, : w], d[:, w:]) for d, (o, w) in zip(turned, pieces)]
    stay, cross = [], []
    for d in done:
        top, low = d[:rows], d[rows:]
        stay.append(lax.ppermute(jnp.where(first, top, low), ("layer", "harm"), handed(True)))
        cross.append(lax.ppermute(jnp.where(first, low, top), ("layer", "harm"), handed(False)))
    parts = []
    for part in range(2):
        halves = []
        for a, b in ((stay, cross), (cross, stay)):
            for s, t, (o, w) in zip(a, b, pieces):
                halves.append(jnp.where(first, s[:, part * w : part * w + w], t[:, part * w : part * w + w]))
        parts.append(jnp.concatenate(halves, 1))
    return jnp.stack(parts, 1)[None]


def solution(mesh):
    in_specs = (
        P(("grating", "layer"), "harm", None, None),
        P(("grating", "layer"), "harm", None, None),
        P(("grating", "layer"), "harm"),
        P(("grating", "layer"), "harm"),
        P(("grating", "layer")),
        P(("grating", "layer")),
    )
    out_specs = P(("grating", "layer"), "harm", None, None)
    return jax.shard_map(
        on_device, mesh=mesh, in_specs=in_specs, out_specs=out_specs, check_vma=False
    )
```
